32 devices in a mesh: dp: 8 (over z, y), mp: 4 (over x, core).
Axes of the slice: x: 2, y: 2, z: 4, core: 2. Of those that a mesh axis runs over, the one named last changes fastest.
Arguments:
- hidden_input: bfloat16 [8192, 24], P('dp'), may hold values from -6 to 6
- output_cotangent: bfloat16 [8192, 8192], P('dp', 'mp'), may hold values from -0.023925781 to 0.023925781
- master_weights: float32 [24, 8192], P('dp', 'mp'), may hold values from -6 to 6
- first_codes: int32 [24, 8192], P('dp', 'mp'), may hold values from 0 to 15
- second_codes: int32 [24, 8192], P('dp', 'mp'), may hold values from 0 to 15
- first_rows: float32 [24], P('dp'), may hold values from 0.001 to 0.03
- first_cols: float32 [8192], P('mp'), may hold values from 0.001 to 0.03
- second_rows: float32 [24], P('dp'), may hold values from 1e-05 to 0.001
- second_cols: float32 [8192], P('mp'), may hold values from 1e-05 to 0.001
- step_count: int32 [], replicated, may hold values from 1 to 9
Outputs:
- new_master: float32 [24, 8192], P('dp', 'mp')
- update_ratio: float32 [24, 8192], P('dp', 'mp')
- gathered_params: bfloat16 [24, 8192], P(None, 'mp')
- first_scaled: float32 [24, 8192], P('dp', 'mp')
- second_scaled: float32 [24, 8192], P('dp', 'mp')
- new_first_rows: float32 [24], P('dp')
- new_first_cols: float32 [8192], P('mp')
- new_second_rows: float32 [24], P('dp')
- new_second_cols: float32 [8192], P('mp')
The draws below stay inside these ranges and needn't reach their ends.
All inputs are finite; a program needn't handle non-finite values.
Results may differ from the reference program's by a relative error of at most 0.001.
Values may be sent and summed in bfloat16 or wider, within the bound.
No kernel may reach another device: no remote copies, remote signals or barrier semaphores. Data moves between devices by JAX's collectives and lax.ppermute only.
A program may use at most 64 MiB of HBM per device.

```python
import math
import jax
import jax.numpy as jnp
from jax import lax

D = 8192
ROWS = 24
TOKENS = 8192


def plant(values, own_key, low, high):
    longest = values.shape.index(max(values.shape))
    spots = []
    for shift in (0, 1):
        where = [jax.random.randint(jax.random.fold_in(own_key, axis), (), 0, length) for axis, length in enumerate(values.shape)]
        where[longest] = (where[longest] + shift) % values.shape[longest]
        spots.append(tuple(where))
    return values.at[spots[0]].set(low).at[spots[1]].set(high)


def spiked(values, own_key, source, target, parts, factor):
    def block_of(axis_at):
        return (jnp.arange(values.shape[axis_at]) // (values.shape[axis_at] // parts)).reshape((-1,) + (1,) * (values.ndim - 1 - axis_at))

    one_side = jax.random.permutation(own_key, parts)[block_of(target)]
    far = (block_of(target) + parts // 2) % parts
    return jnp.where((block_of(source) == one_side) | (block_of(source) == far), factor * values, values)


def block_scale(key, extent, pieces, smallest, high):
    loudness, own = 1.0, jax.random.fold_in(key, 6)
    for axis_at, parts in pieces:
        draws = jnp.exp(jax.random.uniform(jax.random.fold_in(own, axis_at), (parts,), jnp.float32, smallest / len(pieces), high / len(pieces)))
        loudness = loudness * jnp.repeat(draws, extent[axis_at] // parts).reshape([-1 if axis == axis_at else 1 for axis in range(len(extent))])
    return loudness


def bell_draw(stream_key, dims, deviation, most, split=(), kind=jnp.bfloat16):
    values = jax.random.normal(stream_key, dims, jnp.float32) * deviation
    if len(split) > 0:
        values = block_scale(stream_key, dims, split, -0.22, 0.18) * values
    return jnp.clip(values, min=-most, max=most).astype(kind)


def noise_with(own_key, extent, deviation, reach, shards, heavy, dtype=jnp.bfloat16):
    result = deviation * jax.random.normal(own_key, extent, jnp.float32)
    if shards:
        result = result * block_scale(own_key, extent, shards, -0.22, 0.18)
    return jnp.clip(spiked(result, jax.random.fold_in(own_key, 3), *heavy), -reach, reach).astype(dtype)


def setup_inputs(seed: int = 0) -> dict:
    splits = jax.random.split(jax.random.key(seed), 11)
    return {
        "hidden_input": noise_with(splits[0], (TOKENS, ROWS), 1.0, 6.0, ((0, 8),), (0, 1, 8, 2.0)),
        "output_cotangent": bell_draw(splits[1], (TOKENS, D), 0.004, 0.023925781, ((0, 8), (1, 4))),
        "master_weights": bell_draw(splits[2], (ROWS, D), 1.0, 6.0, ((0, 8), (1, 4)), jnp.float32),
        "first_codes": plant(jax.random.randint(splits[3], (ROWS, D), 0, 16), jax.random.fold_in(splits[3], 1), 0, 15).astype(jnp.int32),
        "second_codes": plant(jax.random.randint(splits[4], (ROWS, D), 0, 16), jax.random.fold_in(splits[4], 1), 0, 15).astype(jnp.int32),
        "first_rows": jnp.clip(jnp.exp(math.log(0.03) - 3.4011973 * jax.random.uniform(splits[5], (ROWS,), jnp.float32) ** block_scale(splits[5], (ROWS,), ((0, 8),), -0.2, 0.2)), 0.001, 0.03),
        "first_cols": jnp.clip(jnp.exp(math.log(0.03) - 3.4011973 * jax.random.uniform(splits[6], (D,), jnp.float32) ** block_scale(splits[6], (D,), ((0, 4),), -0.2, 0.2)), 0.001, 0.03),
        "second_rows": jnp.clip(jnp.exp(math.log(0.001) - 4.6051703 * jax.random.uniform(splits[7], (ROWS,), jnp.float32) ** block_scale(splits[7], (ROWS,), ((0, 8),), -0.2, 0.2)), 9.999999747378752e-06, 0.001),
        "second_cols": jnp.clip(jnp.exp(math.log(0.001) - 4.6051703 * jax.random.uniform(splits[8], (D,), jnp.float32) ** block_scale(splits[8], (D,), ((0, 4),), -0.2, 0.2)), 9.999999747378752e-06, 0.001),
        "step_count": jax.random.randint(splits[9], (), 1, 10).astype(jnp.int32),
    }


def reference(hidden_input, output_cotangent, master_weights, first_codes, second_codes, first_rows, first_cols, second_rows, second_cols, step_count):
    gradient = jnp.dot(hidden_input.T, output_cotangent, preferred_element_type=jnp.float32)
    entries = gradient.shape[0] * gradient.shape[1]
    gnorm = jnp.sqrt(jnp.sum(gradient * gradient))
    clipf = jnp.minimum(1.0, 0.01 * jnp.sqrt(jnp.float32(entries)) / (gnorm + 1e-06))
    clipped = clipf * gradient
    first_old = (first_codes.astype(jnp.float32) - 7.5) / 7.5 * jnp.minimum(first_rows[:, None], first_cols[None, :])
    second_level = (second_codes.astype(jnp.float32) + 1.0) / 16.0
    second_old = second_level * second_level * jnp.minimum(second_rows[:, None], second_cols[None, :])
    first_new = 0.9 * first_old + 0.1 * clipped
    second_new = 0.95 * second_old + 0.05 * clipped * clipped
    steps = step_count.astype(jnp.float32)
    first_fix = 1.0 - jnp.power(jnp.float32(0.9), steps)
    second_fix = 1.0 - jnp.power(jnp.float32(0.95), steps)
    update_ratio = first_new / first_fix / (jnp.sqrt(second_new / second_fix) + 1e-08)
    new_master = master_weights - 0.001 * (update_ratio + 0.1 * master_weights)
    first_abs = jnp.abs(first_new)
    new_first_rows = lax.optimization_barrier(jnp.max(first_abs, axis=1))
    new_first_cols = lax.optimization_barrier(jnp.max(first_abs, axis=0))
    new_second_rows = lax.optimization_barrier(jnp.max(second_new, axis=1))
    new_second_cols = lax.optimization_barrier(jnp.max(second_new, axis=0))
    first_scaled = first_new / (jnp.minimum(new_first_rows[:, None], new_first_cols[None, :]) + 1e-08)
    second_scaled = second_new / (jnp.minimum(new_second_rows[:, None], new_second_cols[None, :]) + 1e-08)
    gathered_params = new_master.astype(jnp.bfloat16)
    return (new_master, update_ratio, gathered_params, first_scaled, second_scaled, new_first_rows, new_first_cols, new_second_rows, new_second_cols)
```

```python
import jax
import jax.numpy as jnp
from jax import lax
from jax.sharding import PartitionSpec as P


def partner_masks(count):
    masks = []
    bit = 1
    while bit < count:
        masks.append(bit if bit < 4 else bit + bit // 2)
        bit *= 2
    return masks


def swap(value, axis, mask):
    count = lax.axis_size(axis)
    return lax.ppermute(value, axis, [(k, k ^ mask) for k in range(count)])


def fold(value, axis, masks, combine):
    for mask in masks:
        value = combine(value, swap(value, axis, mask))
    return value


def gather_blocks(block, axis, masks):
    own = lax.axis_index(axis)
    held = block[None]
    bit = 1
    for mask in masks:
        other = swap(held, axis, mask)
        low = (own & bit) == 0
        held = jnp.concatenate([jnp.where(low, held, other), jnp.where(low, other, held)], axis=0)
        bit *= 2
    return held


def shards(
    hidden_input,
    output_cotangent,
    master_weights,
    first_codes,
    second_codes,
    first_rows,
    first_cols,
    second_rows,
    second_cols,
    step_count,
):
    local_rows, local_cols = master_weights.shape
    dp, mp = lax.axis_size("dp"), lax.axis_size("mp")
    dp_masks, mp_masks = partner_masks(dp), partner_masks(mp)
    rows = local_rows * dp
    own = lax.axis_index("dp")

    scales = jnp.pad(
        jnp.concatenate([first_rows, second_rows])[None, :],
        ((0, 0), (0, local_cols - 2 * local_rows)),
    )
    wide = jnp.concatenate([master_weights, scales], axis=0)
    codes = jnp.stack([first_codes, second_codes]).astype(jnp.bfloat16)
    wide = gather_blocks(wide, "dp", dp_masks)
    codes = gather_blocks(codes, "dp", dp_masks)
    all_master = wide[:, :local_rows].reshape(rows, local_cols)
    all_first_rows = wide[:, local_rows, :local_rows].reshape(rows)
    all_second_rows = wide[:, local_rows, local_rows : 2 * local_rows].reshape(rows)
    all_first_codes = codes[:, 0].reshape(rows, local_cols)
    all_second_codes = codes[:, 1].reshape(rows, local_cols)

    half = local_cols // 2
    orders = (dp_masks, dp_masks[1:] + dp_masks[:1])
    pieces = []
    for at, order in enumerate(orders):
        part = jnp.dot(
            hidden_input.T,
            output_cotangent[:, at * half : (at + 1) * half],
            preferred_element_type=jnp.float32,
        )
        pieces.append(fold(part, "dp", order, jnp.add))
    gradient = jnp.concatenate(pieces, axis=1)

    squares = fold(jnp.sum(gradient * gradient), "mp", mp_masks, jnp.add)
    entries = rows * local_cols * mp
    clipf = jnp.minimum(1.0, 0.01 * jnp.sqrt(jnp.float32(entries)) / (jnp.sqrt(squares) + 1e-06))
    clipped = clipf * gradient
    first_old = (
        (all_first_codes.astype(jnp.float32) - 7.5)
        / 7.5
        * jnp.minimum(all_first_rows[:, None], first_cols[None, :])
    )
    second_level = (all_second_codes.astype(jnp.float32) + 1.0) / 16.0
    second_old = (
        second_level
        * second_level
        * jnp.minimum(all_second_rows[:, None], second_cols[None, :])
    )
    first_new = 0.9 * first_old + 0.1 * clipped
    second_new = 0.95 * second_old + 0.05 * clipped * clipped
    first_abs = jnp.abs(first_new)
    new_first_cols = jnp.max(first_abs, axis=0)
    new_second_cols = jnp.max(second_new, axis=0)

    def mine(whole):
        return lax.dynamic_slice_in_dim(whole, own * local_rows, local_rows, axis=0)

    first_mine, second_mine = mine(first_new), mine(second_new)
    row_max = jnp.stack([jnp.max(jnp.abs(first_mine), axis=1), jnp.max(second_mine, axis=1)])
    row_max = fold(row_max, "mp", mp_masks, jnp.maximum)
    new_first_rows, new_second_rows = row_max[0], row_max[1]

    steps = step_count.astype(jnp.float32)
    first_fix = 1.0 - jnp.power(jnp.float32(0.9), steps)
    second_fix = 1.0 - jnp.power(jnp.float32(0.95), steps)
    all_update = first_new / first_fix / (jnp.sqrt(second_new / second_fix) + 1e-08)
    all_new = all_master - 0.001 * (all_update + 0.1 * all_master)
    gathered_params = all_new.astype(jnp.bfloat16)
    update_ratio = mine(all_update)
    new_master = mine(all_new)
    first_scaled = first_mine / (
        jnp.minimum(new_first_rows[:, None], new_first_cols[None, :]) + 1e-08
    )
    second_scaled = second_mine / (
        jnp.minimum(new_second_rows[:, None], new_second_cols[None, :]) + 1e-08
    )
    return (
        new_master,
        update_ratio,
        gathered_params,
        first_scaled,
        second_scaled,
        new_first_rows,
        new_first_cols,
        new_second_rows,
        new_second_cols,
    )


def solution(mesh):
    return jax.shard_map(
        shards,
        mesh=mesh,
        in_specs=(
            P("dp", None),
            P("dp", "mp"),
            P("dp", "mp"),
            P("dp", "mp"),
            P("dp", "mp"),
            P("dp"),
            P("mp"),
            P("dp"),
            P("mp"),
            P(),
        ),
        out_specs=(
            P("dp", "mp"),
            P("dp", "mp"),
            P(None, "mp"),
            P("dp", "mp"),
            P("dp", "mp"),
            P("dp"),
            P("mp"),
            P("dp"),
            P("mp"),
        ),
        check_vma=False,
    )
```

```python
import jax
import jax.numpy as jnp
from jax import lax
from jax.sharding import PartitionSpec as P


def partner_masks(count):
    masks = []
    bit = 1
    while bit < count:
        masks.append(bit if bit < 4 else bit + bit // 2)
        bit *= 2
    return masks


def swap(value, axis, mask):
    count = lax.axis_size(axis)
    return lax.ppermute(value, axis, [(k, k ^ mask) for k in range(count)])


def fold(value, axis, masks, combine):
    for mask in masks:
        value = combine(value, swap(value, axis, mask))
    return value


def join(held, other, own, bit):
    low = (own & bit) == 0
    return jnp.concatenate([jnp.where(low, held, other), jnp.where(low, other, held)], axis=0)


def shards(
    hidden_input,
    output_cotangent,
    master_weights,
    first_codes,
    second_codes,
    first_rows,
    first_cols,
    second_rows,
    second_cols,
    step_count,
):
    local_rows, local_cols = master_weights.shape
    dp, mp = lax.axis_size("dp"), lax.axis_size("mp")
    dp_masks, mp_masks = partner_masks(dp), partner_masks(mp)
    rows = local_rows * dp
    own = lax.axis_index("dp")

    scales = jnp.pad(
        jnp.concatenate([first_rows, second_rows])[None, :],
        ((0, 0), (0, local_cols - 2 * local_rows)),
    )
    wide = jnp.concatenate([master_weights, scales], axis=0)
    codes = jnp.stack([first_codes, second_codes]).astype(jnp.bfloat16)
    gradient = jnp.dot(hidden_input.T, output_cotangent, preferred_element_type=jnp.float32)
    wide, codes = wide[None], codes[None]
    for step, mask in enumerate(dp_masks):
        if step == 0:
            gradient, wide, codes = lax.optimization_barrier((gradient, wide, codes))
        gradient = gradient + swap(gradient, "dp", mask)
        wide = join(wide, swap(wide, "dp", mask), own, 1 << step)
        codes = join(codes, swap(codes, "dp", mask), own, 1 << step)
    all_master = wide[:, :local_rows].reshape(rows, local_cols)
    all_first_rows = wide[:, local_rows, :local_rows].reshape(rows)
    all_second_rows = wide[:, local_rows, local_rows : 2 * local_rows].reshape(rows)
    all_first_codes = codes[:, 0].reshape(rows, local_cols)
    all_second_codes = codes[:, 1].reshape(rows, local_cols)

    squares = jnp.sum(gradient * gradient, axis=0, keepdims=True)
    squares = jnp.sum(fold(squares, "mp", mp_masks, jnp.add))
    entries = rows * local_cols * mp
    clipf = jnp.minimum(1.0, 0.01 * jnp.sqrt(jnp.float32(entries)) / (jnp.sqrt(squares) + 1e-06))
    steps = step_count.astype(jnp.float32)
    first_fix = 1.0 - jnp.power(jnp.float32(0.9), steps)
    second_fix = 1.0 - jnp.power(jnp.float32(0.95), steps)

    def moments(grad, first_code, second_code, first_row, second_row):
        clipped = clipf * grad
        first_old = (
            (first_code.astype(jnp.float32) - 7.5)
            / 7.5
            * jnp.minimum(first_row[:, None], first_cols[None, :])
        )
        level = (second_code.astype(jnp.float32) + 1.0) / 16.0
        second_old = level * level * jnp.minimum(second_row[:, None], second_cols[None, :])
        return 0.9 * first_old + 0.1 * clipped, 0.95 * second_old + 0.05 * clipped * clipped

    def stepped(first_new, second_new, master):
        update = first_new / first_fix / (jnp.sqrt(second_new / second_fix) + 1e-08)
        return update, master - 0.001 * (update + 0.1 * master)

    own_gradient = lax.dynamic_slice_in_dim(gradient, own * local_rows, local_rows, axis=0)
    first_mine, second_mine = moments(
        own_gradient, first_codes, second_codes, first_rows, second_rows
    )
    row_max = jnp.stack([jnp.max(jnp.abs(first_mine), axis=1), jnp.max(second_mine, axis=1)])
    row_max = fold(row_max, "mp", mp_masks, jnp.maximum)
    new_first_rows, new_second_rows = row_max[0], row_max[1]
    update_ratio, new_master = stepped(first_mine, second_mine, master_weights)

    first_new, second_new = moments(
        gradient, all_first_codes, all_second_codes, all_first_rows, all_second_rows
    )
    new_first_cols = jnp.max(jnp.abs(first_new), axis=0)
    new_second_cols = jnp.max(second_new, axis=0)
    gathered_params = stepped(first_new, second_new, all_master)[1].astype(jnp.bfloat16)
    first_scaled = first_mine / (
        jnp.minimum(new_first_rows[:, None], new_first_cols[None, :]) + 1e-08
    )
    second_scaled = second_mine / (
        jnp.minimum(new_second_rows[:, None], new_second_cols[None, :]) + 1e-08
    )
    return (
        new_master,
        update_ratio,
        gathered_params,
        first_scaled,
        second_scaled,
        new_first_rows,
        new_first_cols,
        new_second_rows,
        new_second_cols,
    )


def solution(mesh):
    return jax.shard_map(
        shards,
        mesh=mesh,
        in_specs=(
            P("dp", None),
            P("dp", "mp"),
            P("dp", "mp"),
            P("dp", "mp"),
            P("dp", "mp"),
            P("dp"),
            P("mp"),
            P("dp"),
            P("mp"),
            P(),
        ),
        out_specs=(
            P("dp", "mp"),
            P("dp", "mp"),
            P(None, "mp"),
            P("dp", "mp"),
            P("dp", "mp"),
            P("dp"),
            P("mp"),
            P("dp"),
            P("mp"),
        ),
        check_vma=False,
    )
```

```python
import jax
import jax.numpy as jnp
from jax import lax
from jax.sharding import PartitionSpec as P


def partner_masks(count):
    masks = []
    bit = 1
    while bit < count:
        masks.append(bit if bit < 4 else bit + bit // 2)
        bit *= 2
    return masks


def swap(value, axis, mask):
    count = lax.axis_size(axis)
    return lax.ppermute(value, axis, [(k, k ^ mask) for k in range(count)])


def fold(value, axis, masks, combine):
    for mask in masks:
        value = combine(value, swap(value, axis, mask))
    return value


def join(held, other, own, bit):
    low = (own & bit) == 0
    return jnp.concatenate([jnp.where(low, held, other), jnp.where(low, other, held)], axis=0)


def shards(
    hidden_input,
    output_cotangent,
    master_weights,
    first_codes,
    second_codes,
    first_rows,
    first_cols,
    second_rows,
    second_cols,
    step_count,
):
    local_rows, local_cols = master_weights.shape
    dp, mp = lax.axis_size("dp"), lax.axis_size("mp")
    dp_masks, mp_masks = partner_masks(dp), partner_masks(mp)
    rows = local_rows * dp
    own = lax.axis_index("dp")

    scales = jnp.pad(
        jnp.concatenate([first_rows, second_rows])[None, :],
        ((0, 0), (0, local_cols - 2 * local_rows)),
    )
    wide = jnp.concatenate(
        [master_weights, scales, first_codes.astype(jnp.float32), second_codes.astype(jnp.float32)],
        axis=0,
    )
    gradient = jnp.dot(hidden_input.T, output_cotangent, preferred_element_type=jnp.float32)
    wide = wide[None]
    for step, mask in enumerate(dp_masks):
        if step == 0:
            gradient, wide = lax.optimization_barrier((gradient, wide))
        gradient = gradient + swap(gradient, "dp", mask)
        wide = join(wide, swap(wide, "dp", mask), own, 1 << step)
    all_master = wide[:, :local_rows].reshape(rows, local_cols)
    all_first_rows = wide[:, local_rows, :local_rows].reshape(rows)
    all_second_rows = wide[:, local_rows, local_rows : 2 * local_rows].reshape(rows)
    all_first_codes = wide[:, local_rows + 1 : 2 * local_rows + 1].reshape(rows, local_cols)
    all_second_codes = wide[:, 2 * local_rows + 1 :].reshape(rows, local_cols)

    squares = jnp.sum(gradient * gradient, axis=0, keepdims=True)
    squares = jnp.sum(fold(squares, "mp", mp_masks, jnp.add))
    entries = rows * local_cols * mp
    clipf = jnp.minimum(1.0, 0.01 * jnp.sqrt(jnp.float32(entries)) / (jnp.sqrt(squares) + 1e-06))
    steps = step_count.astype(jnp.float32)
    first_fix = 1.0 - jnp.power(jnp.float32(0.9), steps)
    second_fix = 1.0 - jnp.power(jnp.float32(0.95), steps)

    def moments(grad, first_code, second_code, first_row, second_row):
        clipped = clipf * grad
        first_old = (
            (first_code.astype(jnp.float32) - 7.5)
            / 7.5
            * jnp.minimum(first_row[:, None], first_cols[None, :])
        )
        level = (second_code.astype(jnp.float32) + 1.0) / 16.0
        second_old = level * level * jnp.minimum(second_row[:, None], second_cols[None, :])
        return 0.9 * first_old + 0.1 * clipped, 0.95 * second_old + 0.05 * clipped * clipped

    def stepped(first_new, second_new, master):
        update = first_new / first_fix / (jnp.sqrt(second_new / second_fix) + 1e-08)
        return update, master - 0.001 * (update + 0.1 * master)

    own_gradient = lax.dynamic_slice_in_dim(gradient, own * local_rows, local_rows, axis=0)
    first_mine, second_mine = moments(
        own_gradient, first_codes, second_codes, first_rows, second_rows
    )
    row_max = jnp.stack([jnp.max(jnp.abs(first_mine), axis=1), jnp.max(second_mine, axis=1)])
    row_max = fold(row_max, "mp", mp_masks, jnp.maximum)
    new_first_rows, new_second_rows = row_max[0], row_max[1]
    update_ratio, new_master = stepped(first_mine, second_mine, master_weights)

    first_new, second_new = moments(
        gradient, all_first_codes, all_second_codes, all_first_rows, all_second_rows
    )
    new_first_cols = jnp.max(jnp.abs(first_new), axis=0)
    new_second_cols = jnp.max(second_new, axis=0)
    gathered_params = stepped(first_new, second_new, all_master)[1].astype(jnp.bfloat16)
    first_scaled = first_mine / (
        jnp.minimum(new_first_rows[:, None], new_first_cols[None, :]) + 1e-08
    )
    second_scaled = second_mine / (
        jnp.minimum(new_second_rows[:, None], new_second_cols[None, :]) + 1e-08
    )
    return (
        new_master,
        update_ratio,
        gathered_params,
        first_scaled,
        second_scaled,
        new_first_rows,
        new_first_cols,
        new_second_rows,
        new_second_cols,
    )


def solution(mesh):
    return jax.shard_map(
        shards,
        mesh=mesh,
        in_specs=(
            P("dp", None),
            P("dp", "mp"),
            P("dp", "mp"),
            P("dp", "mp"),
            P("dp", "mp"),
            P("dp"),
            P("mp"),
            P("dp"),
            P("mp"),
            P(),
        ),
        out_specs=(
            P("dp", "mp"),
            P("dp", "mp"),
            P(None, "mp"),
            P("dp", "mp"),
            P("dp", "mp"),
            P("dp"),
            P("mp"),
            P("dp"),
            P("mp"),
        ),
        check_vma=False,
    )
```
